128 devices in a mesh: dp: 8 (over z_hi, y), mp: 8 (over z_lo, x), outer: 2 (over core).
Axes of the slice: x: 4, y: 4, z: 4 (z_hi: 2, z_lo: 2; z = z_hi * 2 + z_lo), core: 2. Of those that a mesh axis runs over, the one named last changes fastest.
Arguments:
- activations: bfloat16 [32768, 8192], P(('dp', 'outer'), 'mp'), may hold values from -6 to 6
- act_scale: float32 [256, 64], P(('dp', 'outer'), 'mp'), may hold values from 0.25 to 4
- out_grads: bfloat16 [32768, 16384], P(('dp', 'outer'), 'mp'), may hold values from -6 to 6
- gradient_tile_scale: float32 [256, 128], P(('dp', 'outer'), 'mp'), may hold values from 0.25 to 4
- prior_input_factor: float32 [8, 1024, 1024], P('mp', ('dp', 'outer')), may hold values from -0.3 to 6, as said below
- g_factor: float32 [16, 1024, 1024], P('mp', ('dp', 'outer')), may hold values from -0.3 to 6, as said below
- weight_grad: bfloat16 [8192, 16384], P('mp', ('dp', 'outer')), may hold values from -6 to 6
- a_inverse: bfloat16 [8, 1024, 1024], P('mp', ('dp', 'outer')), as said below
- g_inverse: bfloat16 [16, 1024, 1024], P(('dp', 'outer'), 'mp'), as said below
Outputs:
- a_stat: float32 [8, 1024, 1024], P('mp', ('dp', 'outer'))
- g_stat: float32 [16, 1024, 1024], P('mp', ('dp', 'outer'))
- new_a_factor: float32 [8, 1024, 1024], P('mp', ('dp', 'outer'))
- new_g_factor: float32 [16, 1024, 1024], P('mp', ('dp', 'outer'))
- preconditioned: bfloat16 [8192, 16384], P('mp', ('dp', 'outer'))
The draws below stay inside these ranges and needn't reach their ends.
Inputs may be any that keep to these rules, and one draw needn't show every extreme that they name: `a_inverse`: each block is the identity plus dense off-diagonal and diagonal entries of magnitude at most 1.5 / sqrt(1024). `g_inverse`: each block is the identity plus dense off-diagonal and diagonal entries of magnitude at most 1.5 / sqrt(1024). `prior_input_factor`: each block is symmetric with a positive diagonal. `g_factor`: each block is symmetric with a positive diagonal.
All inputs are finite; a program needn't handle non-finite values.
Results may differ from the reference program's by a relative error of at most 0.014.
Values may be sent and summed in bfloat16 or wider, within the bound.
A program may use at most 128 MiB of HBM per device.

```python
import math
import jax
import jax.numpy as jnp
from jax import lax

D = 8192
HID = 16384
BLK = 1024
QT = 128
TOKENS = 32768


def inverse_blocks(key, block_count):
    limit = 1.5 / math.sqrt(BLK)
    spread_part = jnp.clip(jax.random.normal(key, (block_count, BLK, BLK), jnp.float32) * (0.5 / math.sqrt(BLK)), -limit, limit)
    identity = jnp.eye(BLK, dtype=jnp.float32)
    return (identity[None, :, :] + spread_part).astype(jnp.bfloat16)


def factor_blocks(key, block_count):
    level = (16.0 - 1.0 / 16.0) / (4.0 * math.log(4.0))
    diag_key, off_key = jax.random.split(key)
    diag_part = level * jax.random.uniform(diag_key, (block_count, BLK), jnp.float32, 0.6, 1.6)
    raw = jnp.clip(jax.random.normal(off_key, (block_count, BLK, BLK), jnp.float32) * 0.05, -0.2, 0.2)
    symmetric = (raw + jnp.transpose(raw, (0, 2, 1))) * 0.7
    identity = jnp.eye(BLK, dtype=jnp.float32)
    off_part = symmetric * (1.0 - identity)[None, :, :]
    return off_part + identity[None, :, :] * diag_part[:, :, None]


def draw_a_inverse(key, part):
    return inverse_blocks(jax.random.fold_in(key, 11), D // BLK)


def draw_g_inverse(key, part):
    return inverse_blocks(jax.random.fold_in(key, 23), HID // BLK)


def draw_prior_input_factor(key, part):
    return factor_blocks(jax.random.fold_in(key, 37), D // BLK)


def draw_g_factor(key, part):
    return factor_blocks(jax.random.fold_in(key, 41), HID // BLK)


def levels(own_key, extent, pieces, least, top_value):
    level, own = 1.0, jax.random.fold_in(own_key, 6)
    for axis_at, shards_of in pieces:
        heights = jnp.exp(jax.random.uniform(jax.random.fold_in(own, axis_at), (shards_of,), jnp.float32, least / len(pieces), top_value / len(pieces)))
        level = level * jnp.repeat(heights, extent[axis_at] // shards_of).reshape([-1 if axis == axis_at else 1 for axis in range(len(extent))])
    return level


def scatter_about(own_key, dims, scale, most, cuts=(), kind=jnp.bfloat16):
    level = levels(own_key, dims, cuts, -0.22, 0.18) if cuts else 1.0
    entries = jax.random.normal(own_key, dims, jnp.float32) * scale * level
    return jnp.minimum(jnp.maximum(entries, -most), most).astype(kind)


def setup_inputs(seed: int = 0) -> dict:
    splits = jax.random.split(jax.random.key(seed), 10)
    activations = scatter_about(splits[0], (TOKENS, D), 1.0, 6.0, ((0, 16), (1, 8)))
    act_scale = jnp.clip(jnp.exp(math.log(4.0) - 2.7725887 * jax.random.uniform(splits[1], (TOKENS // QT, D // QT), jnp.float32) ** levels(splits[1], (TOKENS // QT, D // QT), ((0, 16), (1, 8)), -0.2, 0.2)), 0.25, 4.0)
    out_grads = scatter_about(splits[2], (TOKENS, HID), 1.0, 6.0, ((0, 16), (1, 8)))
    gradient_tile_scale = jnp.clip(jnp.exp(math.log(4.0) - 2.7725887 * jax.random.uniform(splits[3], (TOKENS // QT, HID // QT), jnp.float32) ** levels(splits[3], (TOKENS // QT, HID // QT), ((0, 16), (1, 8)), -0.2, 0.2)), 0.25, 4.0)
    prior_input_factor = draw_prior_input_factor(jax.random.fold_in(splits[9], 71), 0)
    g_factor = draw_g_factor(jax.random.fold_in(splits[9], 71), 0)
    weight_grad = scatter_about(splits[6], (D, HID), 1.0, 6.0, ((0, 8), (1, 16)))
    a_inverse = draw_a_inverse(jax.random.fold_in(splits[9], 71), 0)
    g_inverse = draw_g_inverse(jax.random.fold_in(splits[9], 71), 0)
    return {"activations": activations, "act_scale": act_scale, "out_grads": out_grads, "gradient_tile_scale": gradient_tile_scale, "prior_input_factor": prior_input_factor, "g_factor": g_factor, "weight_grad": weight_grad, "a_inverse": a_inverse, "g_inverse": g_inverse}


EMA_DECAY = 0.95


def dequantize(quantized, tile_scale):
    row_total, column_total = quantized.shape
    tiles_with_scale = quantized.astype(jnp.float32).reshape(row_total // QT, QT, column_total // QT, QT) * tile_scale[:, None, :, None]
    return tiles_with_scale.reshape(row_total, column_total).astype(jnp.bfloat16)


def block_grams(unscaled_values):
    blocks = unscaled_values.reshape(unscaled_values.shape[0], -1, BLK).transpose(1, 0, 2)

    def one_gram(block):
        wide = block.astype(jnp.float32)
        return jnp.dot(wide.T, wide, precision=lax.Precision.HIGHEST, preferred_element_type=jnp.float32)

    return lax.map(one_gram, blocks)


def reference(activations, act_scale, out_grads, gradient_tile_scale, prior_input_factor, g_factor, weight_grad, a_inverse, g_inverse):
    a_deq = dequantize(activations, act_scale)
    g_deq = dequantize(out_grads, gradient_tile_scale)
    a_stat = block_grams(a_deq) / TOKENS
    g_stat = block_grams(g_deq) / TOKENS
    new_a_factor = EMA_DECAY * prior_input_factor + (1.0 - EMA_DECAY) * a_stat
    new_g_factor = EMA_DECAY * g_factor + (1.0 - EMA_DECAY) * g_stat
    grad_blocks = weight_grad.reshape(D // BLK, BLK, HID // BLK, BLK).astype(jnp.float32)
    right = jnp.einsum("aigk,gkl->aigl", grad_blocks, g_inverse.astype(jnp.float32), precision=lax.Precision.HIGHEST).astype(jnp.bfloat16)
    result = jnp.einsum("aij,ajgl->aigl", a_inverse.astype(jnp.float32), right.astype(jnp.float32), precision=lax.Precision.HIGHEST).astype(jnp.bfloat16)
    return a_stat, g_stat, new_a_factor, new_g_factor, result.reshape(D, HID)
```

```python
import jax
import jax.numpy as jnp
from jax import lax
from jax.experimental import pallas as pl
from jax.experimental.pallas import tpu as pltpu
from jax.sharding import PartitionSpec as P

BLK = 1024
QT = 128
EMA_DECAY = 0.95

MESH = pl.DeviceIdType.MESH
NB = 3
STRIPS = 8
KEPT = 5
WIDE = KEPT * QT
CHUNK = 256


def kernel(
    act_scale,
    grad_scale,
    act_hbm,
    grads_hbm,
    weight_hbm,
    a_inv_hbm,
    g_inv_hbm,
    a_out,
    g_out,
    pre_out,
    raw,
    deq,
    deq_t,
    parts,
    swapped,
    chip_sums,
    arrived,
    sums,
    mirror_out,
    mirror_in,
    turned,
    g_full,
    a_full,
    weight,
    right,
    load_sem,
    own_sem,
    g_send,
    g_recv,
    a_send,
    a_recv,
    swap_send,
    swap_recv,
    rs_send,
    rs_recv,
    mir_send,
    mir_recv,
):
    dp = lax.axis_index("dp")
    mp = lax.axis_index("mp")
    core = lax.axis_index("outer")
    y = lax.rem(dp, 4)
    x = lax.rem(mp, 4)
    tokens = act_hbm.shape[0]
    chunks = tokens // CHUNK
    tiles = tokens // QT

    def strip_of(offset):
        return lax.rem(dp + offset, STRIPS)

    def y_peer(offset):
        return dp - y + lax.rem(y + offset, 4)

    def x_peer(offset):
        return mp - x + lax.rem(x + offset, 4)

    def z_far(index):
        return lax.rem(index + 4, 8)

    def load(b, k):
        rows = pl.ds(pl.multiple_of(k * CHUNK, CHUNK), CHUNK)
        if b == 0:
            source = act_hbm.at[rows, :]
        else:
            source = grads_hbm.at[rows, pl.ds((b - 1) * BLK, BLK)]
        return pltpu.make_async_copy(source, raw.at[b, rows, :], load_sem.at[b, k])

    def g_rows(slot):
        return g_full.at[pl.ds(pl.multiple_of(slot * 128, 128), 128), :]

    def a_rows(strip, half):
        return a_full.at[pl.ds(pl.multiple_of(strip * 128 + half * 64, 64), 64), :]

    own_g = pltpu.make_async_copy(g_inv_hbm.at[0], g_rows(mp), own_sem.at[0])
    own_a = pltpu.make_async_copy(a_inv_hbm.at[0], a_rows(dp, core), own_sem.at[1])
    own_w = pltpu.make_async_copy(weight_hbm, weight, own_sem.at[2])
    own_g.start()
    own_a.start()
    for k in range(chunks):
        load(0, k).start()

    barrier = pltpu.get_barrier_semaphore()
    for offset in range(STRIPS):
        for other in range(2):
            if (offset, other) != (0, 0):
                pl.semaphore_signal(
                    barrier,
                    inc=1,
                    device_id={"dp": strip_of(offset), "outer": lax.rem(core + other, 2)},
                    device_id_type=MESH,
                )
    for offset in (1, 2, 3):
        pl.semaphore_signal(barrier, inc=1, device_id={"mp": x_peer(offset)}, device_id_type=MESH)
    pl.semaphore_signal(barrier, inc=1, device_id={"mp": z_far(mp)}, device_id_type=MESH)
    for b in (1, 2):
        for k in range(chunks):
            load(b, k).start()
    own_w.start()
    own_g.wait()
    own_a.wait()
    pl.semaphore_wait(barrier, 2 * STRIPS - 1 + 4)

    def g_copy(slot, kind, peer):
        rows = g_rows(slot)
        return pltpu.make_async_remote_copy(
            rows, rows, g_send.at[kind], g_recv.at[kind],
            device_id={"mp": peer}, device_id_type=MESH,
        )

    def a_copy(strip, half, kind, peer):
        rows = a_rows(strip, half)
        return pltpu.make_async_remote_copy(
            rows, rows, a_send.at[kind], a_recv.at[kind],
            device_id=peer, device_id_type=MESH,
        )

    g_far = g_copy(mp, 0, z_far(mp))
    a_far = a_copy(dp, core, 0, {"dp": z_far(dp)})
    g_near = [g_copy(mp, o, x_peer(o)) for o in (1, 2, 3)]
    a_near = [a_copy(dp, core, o, {"dp": y_peer(o)}) for o in (1, 2, 3)]
    a_pair = [a_copy(dp, core, 7, {"outer": 1 - core})]
    g_far.start()
    a_far.start()
    for o in (0, 2, 1):
        g_near[o].start()
        a_near[o].start()
    a_pair[0].start()
    g_next = [g_copy(z_far(mp), 3 + o, x_peer(o)) for o in (1, 2, 3)]
    a_next = [a_copy(z_far(dp), core, 3 + o, {"dp": y_peer(o)}) for o in (1, 2, 3)]

    def dequantize(b):
        def one(k, carry):
            rows = pl.ds(pl.multiple_of(k * QT, QT), QT)
            for t in range(BLK // QT):
                scale = jnp.where(
                    b == 0, act_scale[k, t], grad_scale[k, jnp.maximum(b - 1, 0) * 8 + t]
                )
                cols = slice(t * QT, (t + 1) * QT)
                value = (raw[b, rows, cols].astype(jnp.float32) * scale).astype(jnp.bfloat16)
                deq[rows, cols] = value
                flipped = value.T
                deq_t[(t + 4) * QT : (t + 5) * QT, rows] = flipped
                if t >= 4:
                    deq_t[(t - 4) * QT : (t - 3) * QT, rows] = flipped
            return carry

        def group(g, carry):
            for bb in range(NB):
                @pl.when(b == bb)
                def _():
                    load(bb, g).wait()

            return lax.fori_loop(g * (CHUNK // QT), (g + 1) * (CHUNK // QT), one, carry)

        lax.fori_loop(0, chunks, group, 0)

    def gram(b):
        def one(j, carry):
            lhs = deq_t[pl.ds(pl.multiple_of(j * 256, 256), 768), :]
            rhs = deq[:, pl.ds(pl.multiple_of(j * 256, 256), 256)]
            tile = jnp.dot(lhs, rhs, preferred_element_type=jnp.float32).astype(jnp.bfloat16)
            for i in range(6):
                strip = lax.rem(2 * j + 4 + i, STRIPS)
                for t in range(2):
                    d = 4 - i + t
                    if 0 <= d < KEPT:
                        for half in range(2):
                            top = i * QT + half * 64
                            parts[half, b, strip, :, d * QT : (d + 1) * QT] = tile[
                                top : top + 64, t * QT : (t + 1) * QT
                            ]
            return carry

        lax.fori_loop(0, 4, one, 0)

    def swap(b):
        return pltpu.make_async_remote_copy(
            parts.at[1 - core, b], swapped.at[b], swap_send.at[b], swap_recv.at[b],
            device_id={"outer": 1 - core}, device_id_type=MESH,
        )

    def scatter(b, offset):
        return pltpu.make_async_remote_copy(
            chip_sums.at[b, strip_of(offset)], arrived.at[offset - 1, b],
            rs_send.at[b, offset - 1], rs_recv.at[b, offset - 1],
            device_id={"dp": strip_of(offset)}, device_id_type=MESH,
        )

    def chip_sum(b):
        swap(b).wait()

        def one(q, carry):
            total = parts[core, b, q].astype(jnp.float32) + swapped[b, q].astype(jnp.float32)
            chip_sums[b, q] = total.astype(jnp.bfloat16)
            return carry

        lax.fori_loop(0, STRIPS, one, 0)
        for offset in (4, 1, 3, 5, 7, 2, 6):
            scatter(b, offset).start()

    def block(b, carry):
        dequantize(b)

        @pl.when(b > 0)
        def _():
            chip_sum(b - 1)

        gram(b)
        swap(b).start()

        @pl.when(b == 0)
        def _():
            g_far.wait()
            a_far.wait()
            for o in (0, 2, 1):
                g_next[o].start()
                a_next[o].start()

        return carry

    lax.fori_loop(0, NB, block, 0)
    chip_sum(NB - 1)

    a_pair.append(a_copy(z_far(dp), core, 8, {"outer": 1 - core}))
    a_pair[-1].start()
    for o in (1, 2, 3):
        a_near[o - 1].wait()
        a_pair.append(a_copy(y_peer(4 - o), core, 8 + o, {"outer": 1 - core}))
        a_pair[-1].start()
    for o in (1, 2, 3):
        a_next[o - 1].wait()
        a_pair.append(a_copy(z_far(y_peer(4 - o)), core, 11 + o, {"outer": 1 - core}))
        a_pair[-1].start()
    for o in (1, 2, 3):
        g_near[o - 1].wait()
        g_next[o - 1].wait()
    for copy in a_pair:
        copy.wait()
    own_w.wait()

    def precondition(n, carry):
        cols = pl.ds(pl.multiple_of(n * 256, 256), 256)
        right[...] = jnp.dot(
            weight[...], g_full[:, cols], preferred_element_type=jnp.float32
        ).astype(jnp.bfloat16)
        pre_out[:, cols] = jnp.dot(
            a_full[...], right[...], preferred_element_type=jnp.float32
        ).astype(jnp.bfloat16)
        return carry

    lax.fori_loop(0, 4, precondition, 0)

    def mirror(b, d, other):
        to_core = lax.rem(core + other, 2)
        return pltpu.make_async_remote_copy(
            mirror_out.at[b, d - 1],
            mirror_in.at[b, d - 1, pl.ds(pl.multiple_of(core * 64, 64), 64), :],
            mir_send.at[b, d - 1, other], mir_recv.at[b, d - 1, other],
            device_id={"dp": strip_of(d), "outer": to_core}, device_id_type=MESH,
        )

    def finish(b, carry):
        for offset in range(1, STRIPS):
            scatter(b, offset).wait()
        total = chip_sums[b, dp].astype(jnp.float32)
        for offset in range(1, STRIPS):
            total = total + arrived[offset - 1, b].astype(jnp.float32)
        for d in range(KEPT):
            cols = pl.ds(pl.multiple_of(strip_of(d) * QT, QT), QT)
            piece = total[:, d * QT : (d + 1) * QT]
            sums[b, :, cols] = piece
            if 1 <= d <= 3:
                mirror_out[b, d - 1] = piece.astype(jnp.bfloat16)
        for d in (1, 2, 3):
            for other in range(2):
                mirror(b, d, other).start()
        return carry

    lax.fori_loop(0, NB, finish, 0)

    def last(b, carry):
        for d in (1, 2, 3):
            for other in range(2):
                mirror(b, d, other).wait()
        for d in (1, 2, 3):
            turned[...] = mirror_in[b, d - 1].astype(jnp.float32).T
            cols = pl.ds(pl.multiple_of(strip_of(STRIPS - d) * QT, QT), QT)
            sums[b, :, cols] = turned[pl.ds(pl.multiple_of(core * 64, 64), 64), :]
        return carry

    lax.fori_loop(0, NB, last, 0)
    a_out[0] = sums[0]
    g_out[0] = sums[1]
    g_out[1] = sums[2]


def body(
    activations,
    act_scale,
    out_grads,
    gradient_tile_scale,
    prior_input_factor,
    g_factor,
    weight_grad,
    a_inverse,
    g_inverse,
):
    tokens = activations.shape[0]
    token_total = tokens * lax.axis_size("dp") * lax.axis_size("outer")
    vmem = pl.BlockSpec(memory_space=pltpu.VMEM)
    smem = pl.BlockSpec(memory_space=pltpu.SMEM)
    anywhere = pl.BlockSpec(memory_space=pl.ANY)
    bf16, f32 = jnp.bfloat16, jnp.float32
    dma = pltpu.SemaphoreType.DMA
    a_sum, g_sum, preconditioned = pl.pallas_call(
        kernel,
        out_shape=(
            jax.ShapeDtypeStruct((1, 64, BLK), f32),
            jax.ShapeDtypeStruct((2, 64, BLK), f32),
            jax.ShapeDtypeStruct((BLK, BLK), bf16),
        ),
        in_specs=[smem, smem] + [anywhere] * 5,
        out_specs=(vmem, vmem, vmem),
        scratch_shapes=[
            pltpu.VMEM((NB, tokens, BLK), bf16),
            pltpu.VMEM((tokens, BLK), bf16),
            pltpu.VMEM((12 * QT, tokens), bf16),
            pltpu.VMEM((2, NB, STRIPS, 64, WIDE), bf16),
            pltpu.VMEM((NB, STRIPS, 64, WIDE), bf16),
            pltpu.VMEM((NB, STRIPS, 64, WIDE), bf16),
            pltpu.VMEM((STRIPS - 1, NB, 64, WIDE), bf16),
            pltpu.VMEM((NB, 64, BLK), f32),
            pltpu.VMEM((NB, 3, 64, QT), bf16),
            pltpu.VMEM((NB, 3, QT, QT), bf16),
            pltpu.VMEM((QT, QT), f32),
            pltpu.VMEM((BLK, BLK), bf16),
            pltpu.VMEM((BLK, BLK), bf16),
            pltpu.VMEM((BLK, BLK), bf16),
            pltpu.VMEM((BLK, 256), bf16),
            dma((NB, tokens // CHUNK)),
            dma((3,)),
            dma((7,)),
            dma((7,)),
            dma((15,)),
            dma((15,)),
            dma((NB,)),
            dma((NB,)),
            dma((NB, STRIPS - 1)),
            dma((NB, STRIPS - 1)),
            dma((NB, 3, 2)),
            dma((NB, 3, 2)),
        ],
        compiler_params=pltpu.CompilerParams(
            collective_id=0, has_side_effects=True, vmem_limit_bytes=56 << 20
        ),
        cost_estimate=pl.CostEstimate(
            flops=14_000_000_000, bytes_accessed=20_000_000, transcendentals=0
        ),
    )(
        act_scale,
        gradient_tile_scale,
        activations,
        out_grads,
        weight_grad,
        a_inverse,
        g_inverse,
    )
    a_stat = a_sum / token_total
    g_stat = g_sum / token_total
    new_a_factor = EMA_DECAY * prior_input_factor + (1.0 - EMA_DECAY) * a_stat
    new_g_factor = EMA_DECAY * g_factor + (1.0 - EMA_DECAY) * g_stat
    return a_stat, g_stat, new_a_factor, new_g_factor, preconditioned


def solution(mesh):
    return jax.shard_map(
        body,
        mesh=mesh,
        in_specs=(
            P(("dp", "outer"), "mp"),
            P(("dp", "outer"), "mp"),
            P(("dp", "outer"), "mp"),
            P(("dp", "outer"), "mp"),
            P("mp", ("dp", "outer"), None),
            P("mp", ("dp", "outer"), None),
            P("mp", ("dp", "outer")),
            P("mp", ("dp", "outer"), None),
            P(("dp", "outer"), "mp", None),
        ),
        out_specs=(
            P("mp", ("dp", "outer"), None),
            P("mp", ("dp", "outer"), None),
            P("mp", ("dp", "outer"), None),
            P("mp", ("dp", "outer"), None),
            P("mp", ("dp", "outer")),
        ),
        check_vma=False,
    )
```

```python
import functools

import jax
import jax.numpy as jnp
from jax import lax
from jax.experimental import pallas as pl
from jax.experimental.pallas import tpu as pltpu
from jax.sharding import PartitionSpec as P

BLK = 1024
QT = 128
EMA_DECAY = 0.95

MESH = pl.DeviceIdType.MESH
NB = 3
STRIPS = 8
KEPT = 5
WIDE = KEPT * QT
AROUND = (1, 3, 2)
CHUNK = 512


def kernel(
    act_scale_hbm,
    grad_scale_hbm,
    act_hbm,
    grads_hbm,
    weight_hbm,
    a_inv_hbm,
    g_inv_hbm,
    a_out,
    g_out,
    pre_out,
    act_scale,
    grad_scale,
    raw,
    deq_even,
    deq_odd,
    flip_even,
    flip_odd,
    parts,
    swapped,
    chip_sums,
    first_in,
    middle,
    second_in,
    own_sum,
    sums,
    mirror_out,
    mirror_in,
    turned,
    g_full,
    a_full,
    weight,
    right,
    load_sem,
    own_sem,
    g_send,
    g_recv,
    a_send,
    a_recv,
    swap_send,
    swap_recv,
    first_send,
    first_recv,
    second_send,
    second_recv,
    mir_send,
    mir_recv,
):
    dp = lax.axis_index("dp")
    mp = lax.axis_index("mp")
    core = lax.axis_index("outer")
    y = lax.rem(dp, 4)
    x = lax.rem(mp, 4)
    z_half = dp // 4
    tokens = act_hbm.shape[0]
    chunks = tokens // CHUNK
    tiles = tokens // QT

    def strip_of(offset):
        return lax.rem(dp + offset, STRIPS)

    def y_peer(offset):
        return dp - y + lax.rem(y + offset, 4)

    def x_peer(offset):
        return mp - x + lax.rem(x + offset, 4)

    def z_far(index):
        return lax.rem(index + 4, 8)

    def load(b, k):
        rows = pl.ds(pl.multiple_of(k * CHUNK, CHUNK), CHUNK)
        if b == 0:
            source = act_hbm.at[rows, :]
        else:
            source = grads_hbm.at[rows, pl.ds((b - 1) * BLK, BLK)]
        return pltpu.make_async_copy(source, raw.at[b % 2, rows, :], load_sem.at[b, k])

    def g_rows(slot):
        return g_full.at[pl.ds(pl.multiple_of(slot * 128, 128), 128), :]

    def a_rows(strip, half):
        return a_full.at[pl.ds(pl.multiple_of(strip * 128 + half * 64, 64), 64), :]

    own_g = pltpu.make_async_copy(g_inv_hbm.at[0], g_rows(mp), own_sem.at[0])
    own_a = pltpu.make_async_copy(a_inv_hbm.at[0], a_rows(dp, core), own_sem.at[1])
    own_w = pltpu.make_async_copy(weight_hbm, weight, own_sem.at[2])
    own_scales = (
        pltpu.make_async_copy(act_scale_hbm, act_scale, own_sem.at[3]),
        pltpu.make_async_copy(grad_scale_hbm, grad_scale, own_sem.at[4]),
    )
    for copy in own_scales:
        copy.start()
    own_g.start()
    own_a.start()
    for k in range(chunks):
        load(0, k).start()

    barrier = pltpu.get_barrier_semaphore()
    for offset in range(STRIPS):
        for other in range(2):
            if (offset, other) != (0, 0):
                pl.semaphore_signal(
                    barrier,
                    inc=1,
                    device_id={"dp": strip_of(offset), "outer": lax.rem(core + other, 2)},
                    device_id_type=MESH,
                )
    for offset in (1, 2, 3):
        pl.semaphore_signal(barrier, inc=1, device_id={"mp": x_peer(offset)}, device_id_type=MESH)
    pl.semaphore_signal(barrier, inc=1, device_id={"mp": z_far(mp)}, device_id_type=MESH)
    for k in range(chunks):
        load(1, k).start()
    own_w.start()
    own_g.wait()
    own_a.wait()
    for copy in own_scales:
        copy.wait()
    pl.semaphore_wait(barrier, 2 * STRIPS - 1 + 4)

    def g_copy(slot, kind, peer):
        rows = g_rows(slot)
        return pltpu.make_async_remote_copy(
            rows, rows, g_send.at[kind], g_recv.at[kind],
            device_id={"mp": peer}, device_id_type=MESH,
        )

    def a_copy(strip, half, kind, peer):
        rows = a_rows(strip, half)
        return pltpu.make_async_remote_copy(
            rows, rows, a_send.at[kind], a_recv.at[kind],
            device_id=peer, device_id_type=MESH,
        )

    g_far = g_copy(mp, 0, z_far(mp))
    a_far = a_copy(dp, core, 0, {"dp": z_far(dp)})
    g_near = [g_copy(mp, o, x_peer(o)) for o in (1, 2, 3)]
    a_near = [a_copy(dp, core, o, {"dp": y_peer(o)}) for o in (1, 2, 3)]
    a_pair = [a_copy(dp, core, 7, {"outer": 1 - core})]
    a_far.start()
    g_far.start()
    for o in (0, 2, 1):
        g_near[o].start()
        a_near[o].start()
    a_pair[0].start()
    g_next = [g_copy(z_far(mp), 3 + o, x_peer(o)) for o in (1, 2, 3)]
    a_next = [a_copy(z_far(dp), core, 3 + o, {"dp": y_peer(o)}) for o in (1, 2, 3)]

    deqs = (deq_even, deq_odd)
    flips = (flip_even, flip_odd)

    def dequantize(b, k):
        for inner in range(CHUNK // QT):
            tile_row = k * (CHUNK // QT) + inner
            rows = pl.ds(pl.multiple_of(tile_row * QT, QT), QT)
            for t in range(BLK // QT):
                scale = act_scale[t, tile_row] if b == 0 else grad_scale[tile_row, (b - 1) * 8 + t]
                cols = slice(t * QT, (t + 1) * QT)
                value = (raw[b % 2, rows, cols].astype(jnp.float32) * scale).astype(jnp.bfloat16)
                deqs[b % 2][rows, cols] = value
                flipped = value.T
                flips[b % 2][(t + 4) * QT : (t + 5) * QT, rows] = flipped
                if t >= 4:
                    flips[b % 2][(t - 4) * QT : (t - 3) * QT, rows] = flipped

    def gram(b, j):
        lhs = flips[b % 2][pl.ds(pl.multiple_of(j * 256, 256), 768), :]
        rhs = deqs[b % 2][:, pl.ds(pl.multiple_of(j * 256, 256), 256)]
        tile = jnp.dot(lhs, rhs, preferred_element_type=jnp.float32).astype(jnp.bfloat16)
        for i in range(6):
            strip = lax.rem(2 * j + 4 + i, STRIPS)
            for t in range(2):
                d = 4 - i + t
                if 0 <= d < KEPT:
                    for half in range(2):
                        top = i * QT + half * 64
                        parts[half, b, strip, :, d * QT : (d + 1) * QT] = tile[
                            top : top + 64, t * QT : (t + 1) * QT
                        ]

    def swap(b):
        return pltpu.make_async_remote_copy(
            parts.at[1 - core, b], swapped.at[b], swap_send.at[b], swap_recv.at[b],
            device_id={"outer": 1 - core}, device_id_type=MESH,
        )

    def first_ring(b, o):
        return pltpu.make_async_remote_copy(
            chip_sums.at[b, :, lax.rem(y + o, 4)], first_in.at[b, pl.ds(2 * (o - 1), 2)],
            first_send.at[b, o - 1], first_recv.at[b, o - 1],
            device_id={"dp": y_peer(o)}, device_id_type=MESH,
        )

    def first_far(b):
        return pltpu.make_async_remote_copy(
            chip_sums.at[b, 1 - z_half], first_in.at[b, pl.ds(0, 4)],
            first_send.at[b, 3], first_recv.at[b, 3],
            device_id={"dp": z_far(dp)}, device_id_type=MESH,
        )

    def second_ring(b, o):
        return pltpu.make_async_remote_copy(
            middle.at[b, o], second_in.at[b, o - 1],
            second_send.at[b, o - 1], second_recv.at[b, o - 1],
            device_id={"dp": y_peer(o)}, device_id_type=MESH,
        )

    def second_far(b):
        return pltpu.make_async_remote_copy(
            middle.at[b, 1], second_in.at[b, 0], second_send.at[b, 3], second_recv.at[b, 3],
            device_id={"dp": z_far(dp)}, device_id_type=MESH,
        )

    def wide(value):
        return value.astype(jnp.float32)

    def chip_sum(b):
        swap(b).wait()

        def one(q, carry):
            total = wide(parts[core, b, q]) + wide(swapped[b, q])
            chip_sums[b, q // 4, lax.rem(q, 4)] = total.astype(jnp.bfloat16)
            return carry

        lax.fori_loop(0, STRIPS, one, 0)

        @pl.when(core == 0)
        def _():
            for o in AROUND:
                first_ring(b, o).start()

        @pl.when(core == 1)
        def _():
            first_far(b).start()

    def second(b):
        @pl.when(core == 0)
        def _():
            for o in AROUND:
                first_ring(b, o).wait()
            for slot, half in ((1, 1 - z_half), (0, z_half)):
                total = wide(chip_sums[b, half, y])
                for o in AROUND:
                    total = total + wide(first_in[b, 2 * (o - 1) + half])
                middle[b, slot] = total.astype(jnp.bfloat16)
                if slot == 1:
                    second_far(b).start()

        @pl.when(core == 1)
        def _():
            first_far(b).wait()
            for o in (1, 3, 2, 0):
                strip = lax.rem(y + o, 4)
                total = wide(chip_sums[b, z_half, strip]) + wide(first_in[b, strip])
                middle[b, o] = total.astype(jnp.bfloat16)
                if o:
                    second_ring(b, o).start()

    def finish(b):
        @pl.when(core == 0)
        def _():
            second_far(b).wait()
            own_sum[b] = wide(middle[b, 0]) + wide(second_in[b, 0])

        @pl.when(core == 1)
        def _():
            for o in AROUND:
                second_ring(b, o).wait()
            total = wide(middle[b, 0])
            for o in AROUND:
                total = total + wide(second_in[b, o - 1])
            own_sum[b] = total

        for d in range(KEPT):
            cols = pl.ds(pl.multiple_of(strip_of(d) * QT, QT), QT)
            sums[b, :, cols] = own_sum[b, :, d * QT : (d + 1) * QT]

    def mirror(group, d, other):
        to_core = lax.rem(core + other, 2)
        return pltpu.make_async_remote_copy(
            mirror_out.at[group, d - 1, to_core],
            mirror_in.at[group, d - 1, pl.ds(pl.multiple_of(core * 64, 64), 64), :],
            mir_send.at[group, d - 1, other], mir_recv.at[group, d - 1, other],
            device_id={"dp": strip_of(d), "outer": to_core}, device_id_type=MESH,
        )

    def send_mirror(group):
        low = lax.broadcasted_iota(jnp.int32, (64, QT), 1) < 64
        for d in (1, 2, 3):
            cols = slice(d * QT, (d + 1) * QT)
            if group == 0:
                one, two = own_sum[0, :, cols], own_sum[1, :, cols]
                pair = (
                    jnp.where(low, one, pltpu.roll(two, 64, 1)),
                    jnp.where(low, pltpu.roll(one, 64, 1), two),
                )
            else:
                pair = (own_sum[2, :, cols],) * 2
            for half in range(2):
                mirror_out[group, d - 1, half] = pair[half].astype(jnp.bfloat16)
        for d in (1, 2, 3):
            for other in range(2):
                mirror(group, d, other).start()

    def take_mirror(group):
        for d in (1, 2, 3):
            for other in range(2):
                mirror(group, d, other).wait()
        for d in (1, 2, 3):
            cols = pl.ds(pl.multiple_of(strip_of(STRIPS - d) * QT, QT), QT)
            flipped = wide(mirror_in[group, d - 1]).T
            if group == 0:
                sums[0, :, cols] = flipped[:64]
                sums[1, :, cols] = flipped[64:]
            else:
                turned[...] = flipped
                sums[2, :, cols] = turned[pl.ds(pl.multiple_of(core * 64, 64), 64), :]

    def first(k, carry):
        load(0, k).wait()
        dequantize(0, k)
        return carry

    lax.fori_loop(0, chunks, first, 0)
    for k in range(chunks):
        load(2, k).start()

    for b in range(NB):

        def step(j, carry):
            if b > 0:

                @pl.when(j == 1)
                def _():
                    chip_sum(b - 1)
                    if b == 1:
                        g_far.wait()
                        for o in AROUND:
                            g_next[o - 1].start()
                    else:
                        second(b - 2)

            if b == 0:

                @pl.when(j == 2)
                def _():
                    a_far.wait()
                    for o in (0, 2, 1):
                        a_next[o].start()

            if b + 1 < NB:
                load(b + 1, j).wait()
            gram(b, j)
            if b + 1 < NB:
                dequantize(b + 1, j)
            return carry

        lax.fori_loop(0, 4, step, 0)
        swap(b).start()
    chip_sum(NB - 1)
    second(NB - 2)
    finish(0)

    a_pair.append(a_copy(z_far(dp), core, 8, {"outer": 1 - core}))
    a_pair[-1].start()
    for o in (1, 2, 3):
        a_near[o - 1].wait()
        a_pair.append(a_copy(y_peer(4 - o), core, 8 + o, {"outer": 1 - core}))
        a_pair[-1].start()
    for o in (1, 2, 3):
        a_next[o - 1].wait()
        a_pair.append(a_copy(z_far(y_peer(4 - o)), core, 11 + o, {"outer": 1 - core}))
        a_pair[-1].start()
    for o in (1, 2, 3):
        g_near[o - 1].wait()
        g_next[o - 1].wait()
    for copy in a_pair:
        copy.wait()
    own_w.wait()

    def precondition(n):
        cols = pl.ds(n * 512, 512)
        right[...] = jnp.dot(
            weight[...], g_full[:, cols], preferred_element_type=jnp.float32
        ).astype(jnp.bfloat16)
        pre_out[:, cols] = jnp.dot(
            a_full[...], right[...], preferred_element_type=jnp.float32
        ).astype(jnp.bfloat16)

    precondition(0)
    second(NB - 1)
    finish(1)
    send_mirror(0)
    precondition(1)
    finish(2)
    send_mirror(1)
    take_mirror(0)
    take_mirror(1)
    a_out[0] = sums[0]
    g_out[0] = sums[1]
    g_out[1] = sums[2]


def blend(token_total, a_sum, g_sum, pre, prior, factor, a_stat, g_stat, new_a, new_g, pre_out, sem):
    copy = pltpu.make_async_copy(pre, pre_out, sem)
    copy.start()
    for total, old, stat, new in ((a_sum, prior, a_stat, new_a), (g_sum, factor, g_stat, new_g)):
        mean = total[...] / token_total
        stat[...] = mean
        new[...] = EMA_DECAY * old[...] + (1.0 - EMA_DECAY) * mean
    copy.wait()


def body(
    activations,
    act_scale,
    out_grads,
    gradient_tile_scale,
    prior_input_factor,
    g_factor,
    weight_grad,
    a_inverse,
    g_inverse,
):
    tokens = activations.shape[0]
    token_total = tokens * lax.axis_size("dp") * lax.axis_size("outer")
    vmem = pl.BlockSpec(memory_space=pltpu.VMEM)
    hbm = pl.BlockSpec(memory_space=pltpu.HBM)
    bf16, f32 = jnp.bfloat16, jnp.float32
    dma = pltpu.SemaphoreType.DMA
    a_sum, g_sum, preconditioned = pl.pallas_call(
        kernel,
        out_shape=(
            jax.ShapeDtypeStruct((1, 64, BLK), f32),
            jax.ShapeDtypeStruct((2, 64, BLK), f32),
            jax.ShapeDtypeStruct((BLK, BLK), bf16),
        ),
        in_specs=[hbm] * 7,
        out_specs=(vmem, vmem, vmem),
        scratch_shapes=[
            pltpu.SMEM(act_scale.shape[::-1], f32),
            pltpu.SMEM(gradient_tile_scale.shape, f32),
            pltpu.VMEM((2, tokens, BLK), bf16),
            pltpu.VMEM((tokens, BLK), bf16),
            pltpu.VMEM((tokens, BLK), bf16),
            pltpu.VMEM((12 * QT, tokens), bf16),
            pltpu.VMEM((12 * QT, tokens), bf16),
            pltpu.VMEM((2, NB, STRIPS, 64, WIDE), bf16),
            pltpu.VMEM((NB, STRIPS, 64, WIDE), bf16),
            pltpu.VMEM((NB, 2, 4, 64, WIDE), bf16),
            pltpu.VMEM((NB, 6, 64, WIDE), bf16),
            pltpu.VMEM((NB, 4, 64, WIDE), bf16),
            pltpu.VMEM((NB, 3, 64, WIDE), bf16),
            pltpu.VMEM((NB, 64, WIDE), f32),
            pltpu.VMEM((NB, 64, BLK), f32),
            pltpu.VMEM((2, 3, 2, 64, QT), bf16),
            pltpu.VMEM((2, 3, QT, QT), bf16),
            pltpu.VMEM((QT, QT), f32),
            pltpu.VMEM((BLK, BLK), bf16),
            pltpu.VMEM((BLK, BLK), bf16),
            pltpu.VMEM((BLK, BLK), bf16),
            pltpu.VMEM((BLK, 512), bf16),
            dma((NB, tokens // CHUNK)),
            dma((5,)),
            dma((7,)),
            dma((7,)),
            dma((15,)),
            dma((15,)),
            dma((NB,)),
            dma((NB,)),
            dma((NB, 4)),
            dma((NB, 4)),
            dma((NB, 4)),
            dma((NB, 4)),
            dma((2, 3, 2)),
            dma((2, 3, 2)),
        ],
        compiler_params=pltpu.CompilerParams(
            collective_id=0, has_side_effects=True, vmem_limit_bytes=50 << 20
        ),
        cost_estimate=pl.CostEstimate(
            flops=14_000_000_000, bytes_accessed=20_000_000, transcendentals=0
        ),
    )(
        *(
            pltpu.with_memory_space_constraint(value, pltpu.HBM)
            for value in (
                act_scale.T,
                gradient_tile_scale,
                activations,
                out_grads,
                weight_grad,
                a_inverse,
                g_inverse,
            )
        )
    )
    return pl.pallas_call(
        functools.partial(blend, token_total),
        out_shape=(
            jax.ShapeDtypeStruct((1, 64, BLK), f32),
            jax.ShapeDtypeStruct((2, 64, BLK), f32),
            jax.ShapeDtypeStruct((1, 64, BLK), f32),
            jax.ShapeDtypeStruct((2, 64, BLK), f32),
            jax.ShapeDtypeStruct((BLK, BLK), bf16),
        ),
        in_specs=[vmem] * 5,
        out_specs=(vmem, vmem, vmem, vmem, hbm),
        scratch_shapes=[dma],
        compiler_params=pltpu.CompilerParams(vmem_limit_bytes=8 << 20),
    )(a_sum, g_sum, preconditioned, prior_input_factor, g_factor)


def solution(mesh):
    return jax.shard_map(
        body,
        mesh=mesh,
        in_specs=(
            P(("dp", "outer"), "mp"),
            P(("dp", "outer"), "mp"),
            P(("dp", "outer"), "mp"),
            P(("dp", "outer"), "mp"),
            P("mp", ("dp", "outer"), None),
            P("mp", ("dp", "outer"), None),
            P("mp", ("dp", "outer")),
            P("mp", ("dp", "outer"), None),
            P(("dp", "outer"), "mp", None),
        ),
        out_specs=(
            P("mp", ("dp", "outer"), None),
            P("mp", ("dp", "outer"), None),
            P("mp", ("dp", "outer"), None),
            P("mp", ("dp", "outer"), None),
            P("mp", ("dp", "outer")),
        ),
        check_vma=False,
    )
```

```python
import functools

import jax
import jax.numpy as jnp
from jax import lax
from jax.experimental import pallas as pl
from jax.experimental.pallas import tpu as pltpu
from jax.sharding import PartitionSpec as P

BLK = 1024
QT = 128
EMA_DECAY = 0.95

MESH = pl.DeviceIdType.MESH
NB = 3
STRIPS = 8
KEPT = 5
WIDE = KEPT * QT
AROUND = (1, 3, 2)
RING = slice(0, 2 * QT)
FAR = slice(2 * QT, WIDE)
CHUNK = 512


def kernel(
    act_scale_hbm,
    grad_scale_hbm,
    act_hbm,
    grads_hbm,
    weight_hbm,
    a_inv_hbm,
    g_inv_hbm,
    a_out,
    g_out,
    pre_out,
    act_scale,
    grad_scale,
    raw,
    deq_even,
    deq_odd,
    flip_even,
    flip_odd,
    parts,
    swapped,
    chip_sums,
    ring_in,
    far_in,
    ring_middle,
    far_middle,
    ring_second_in,
    far_second_in,
    own_sum,
    sums,
    mirror_out,
    mirror_in,
    turned,
    g_full,
    a_full,
    weight,
    right,
    load_sem,
    own_sem,
    g_send,
    g_recv,
    a_send,
    a_recv,
    swap_send,
    swap_recv,
    first_send,
    first_recv,
    second_send,
    second_recv,
    mir_send,
    mir_recv,
):
    dp = lax.axis_index("dp")
    mp = lax.axis_index("mp")
    core = lax.axis_index("outer")
    y = lax.rem(dp, 4)
    x = lax.rem(mp, 4)
    z_half = dp // 4
    tokens = act_hbm.shape[0]
    chunks = tokens // CHUNK
    tiles = tokens // QT

    def strip_of(offset):
        return lax.rem(dp + offset, STRIPS)

    def y_peer(offset):
        return dp - y + lax.rem(y + offset, 4)

    def x_peer(offset):
        return mp - x + lax.rem(x + offset, 4)

    def z_far(index):
        return lax.rem(index + 4, 8)

    def load(b, k):
        rows = pl.ds(pl.multiple_of(k * CHUNK, CHUNK), CHUNK)
        if b == 0:
            source = act_hbm.at[rows, :]
        else:
            source = grads_hbm.at[rows, pl.ds((b - 1) * BLK, BLK)]
        return pltpu.make_async_copy(source, raw.at[b % 2, rows, :], load_sem.at[b, k])

    def g_rows(slot):
        return g_full.at[pl.ds(pl.multiple_of(slot * 128, 128), 128), :]

    def a_rows(strip, half):
        return a_full.at[pl.ds(pl.multiple_of(strip * 128 + half * 64, 64), 64), :]

    own_g = pltpu.make_async_copy(g_inv_hbm.at[0], g_rows(mp), own_sem.at[0])
    own_a = pltpu.make_async_copy(a_inv_hbm.at[0], a_rows(dp, core), own_sem.at[1])
    own_w = pltpu.make_async_copy(weight_hbm, weight, own_sem.at[2])
    own_scales = (
        pltpu.make_async_copy(act_scale_hbm, act_scale, own_sem.at[3]),
        pltpu.make_async_copy(grad_scale_hbm, grad_scale, own_sem.at[4]),
    )
    for copy in own_scales:
        copy.start()
    own_g.start()
    own_a.start()
    for k in range(chunks):
        load(0, k).start()

    barrier = pltpu.get_barrier_semaphore()
    for offset in range(STRIPS):
        for other in range(2):
            if (offset, other) != (0, 0):
                pl.semaphore_signal(
                    barrier,
                    inc=1,
                    device_id={"dp": strip_of(offset), "outer": lax.rem(core + other, 2)},
                    device_id_type=MESH,
                )
    for offset in (1, 2, 3):
        pl.semaphore_signal(barrier, inc=1, device_id={"mp": x_peer(offset)}, device_id_type=MESH)
    pl.semaphore_signal(barrier, inc=1, device_id={"mp": z_far(mp)}, device_id_type=MESH)
    for k in range(chunks):
        load(1, k).start()
    own_w.start()
    own_g.wait()
    own_a.wait()
    for copy in own_scales:
        copy.wait()
    pl.semaphore_wait(barrier, 2 * STRIPS - 1 + 4)

    def g_copy(slot, kind, peer):
        rows = g_rows(slot)
        return pltpu.make_async_remote_copy(
            rows, rows, g_send.at[kind], g_recv.at[kind],
            device_id={"mp": peer}, device_id_type=MESH,
        )

    def a_copy(strip, half, kind, peer):
        rows = a_rows(strip, half)
        return pltpu.make_async_remote_copy(
            rows, rows, a_send.at[kind], a_recv.at[kind],
            device_id=peer, device_id_type=MESH,
        )

    g_far = g_copy(mp, 0, z_far(mp))
    a_far = a_copy(dp, core, 0, {"dp": z_far(dp)})
    g_near = [g_copy(mp, o, x_peer(o)) for o in (1, 2, 3)]
    a_near = [a_copy(dp, core, o, {"dp": y_peer(o)}) for o in (1, 2, 3)]
    a_pair = [a_copy(dp, core, 7, {"outer": 1 - core})]
    a_far.start()
    g_far.start()
    for o in (0, 2, 1):
        g_near[o].start()
        a_near[o].start()
    a_pair[0].start()
    g_next = [g_copy(z_far(mp), 3 + o, x_peer(o)) for o in (1, 2, 3)]
    a_next = [a_copy(z_far(dp), core, 3 + o, {"dp": y_peer(o)}) for o in (1, 2, 3)]

    deqs = (deq_even, deq_odd)
    flips = (flip_even, flip_odd)

    def dequantize(b, k):
        for inner in range(CHUNK // QT):
            tile_row = k * (CHUNK // QT) + inner
            rows = pl.ds(pl.multiple_of(tile_row * QT, QT), QT)
            for t in range(BLK // QT):
                scale = act_scale[t, tile_row] if b == 0 else grad_scale[tile_row, (b - 1) * 8 + t]
                cols = slice(t * QT, (t + 1) * QT)
                value = (raw[b % 2, rows, cols].astype(jnp.float32) * scale).astype(jnp.bfloat16)
                deqs[b % 2][rows, cols] = value
                flipped = value.T
                flips[b % 2][(t + 4) * QT : (t + 5) * QT, rows] = flipped
                if t >= 4:
                    flips[b % 2][(t - 4) * QT : (t - 3) * QT, rows] = flipped

    def gram(b, j):
        lhs = flips[b % 2][pl.ds(pl.multiple_of(j * 256, 256), 768), :]
        rhs = deqs[b % 2][:, pl.ds(pl.multiple_of(j * 256, 256), 256)]
        tile = jnp.dot(lhs, rhs, preferred_element_type=jnp.float32).astype(jnp.bfloat16)
        for i in range(6):
            strip = lax.rem(2 * j + 4 + i, STRIPS)
            for t in range(2):
                d = 4 - i + t
                if 0 <= d < KEPT:
                    for half in range(2):
                        top = i * QT + half * 64
                        parts[half, b, strip, :, d * QT : (d + 1) * QT] = tile[
                            top : top + 64, t * QT : (t + 1) * QT
                        ]

    def swap(b):
        return pltpu.make_async_remote_copy(
            parts.at[1 - core, b], swapped.at[b], swap_send.at[b], swap_recv.at[b],
            device_id={"outer": 1 - core}, device_id_type=MESH,
        )

    def first_ring(b, o):
        return pltpu.make_async_remote_copy(
            chip_sums.at[b, :, lax.rem(y + o, 4), :, RING], ring_in.at[b, o - 1],
            first_send.at[b, o - 1], first_recv.at[b, o - 1],
            device_id={"dp": y_peer(o)}, device_id_type=MESH,
        )

    def first_far(b):
        return pltpu.make_async_remote_copy(
            chip_sums.at[b, 1 - z_half, :, :, FAR], far_in.at[b],
            first_send.at[b, 3], first_recv.at[b, 3],
            device_id={"dp": z_far(dp)}, device_id_type=MESH,
        )

    def second_ring(b, o):
        return pltpu.make_async_remote_copy(
            far_middle.at[b, o], far_second_in.at[b, o - 1],
            second_send.at[b, o - 1], second_recv.at[b, o - 1],
            device_id={"dp": y_peer(o)}, device_id_type=MESH,
        )

    def second_far(b):
        return pltpu.make_async_remote_copy(
            ring_middle.at[b, 1], ring_second_in.at[b], second_send.at[b, 3], second_recv.at[b, 3],
            device_id={"dp": z_far(dp)}, device_id_type=MESH,
        )

    def wide(value):
        return value.astype(jnp.float32)

    def chip_sum(b):
        swap(b).wait()

        def one(q, carry):
            total = wide(parts[core, b, q]) + wide(swapped[b, q])
            chip_sums[b, q // 4, lax.rem(q, 4)] = total.astype(jnp.bfloat16)
            return carry

        lax.fori_loop(0, STRIPS, one, 0)

        first_far(b).start()
        for o in AROUND:
            first_ring(b, o).start()

    def second(b):
        for o in AROUND:
            first_ring(b, o).wait()
        for slot, half in ((1, 1 - z_half), (0, z_half)):
            total = wide(chip_sums[b, half, y, :, RING])
            for o in AROUND:
                total = total + wide(ring_in[b, o - 1, half])
            ring_middle[b, slot] = total.astype(jnp.bfloat16)
            if slot == 1:
                second_far(b).start()
        first_far(b).wait()
        for o in (1, 3, 2, 0):
            strip = lax.rem(y + o, 4)
            total = wide(chip_sums[b, z_half, strip, :, FAR]) + wide(far_in[b, strip])
            far_middle[b, o] = total.astype(jnp.bfloat16)
            if o:
                second_ring(b, o).start()

    def finish(b):
        second_far(b).wait()
        own_sum[b, :, RING] = wide(ring_middle[b, 0]) + wide(ring_second_in[b])
        for o in AROUND:
            second_ring(b, o).wait()
        total = wide(far_middle[b, 0])
        for o in AROUND:
            total = total + wide(far_second_in[b, o - 1])
        own_sum[b, :, FAR] = total
        for d in range(KEPT):
            cols = pl.ds(pl.multiple_of(strip_of(d) * QT, QT), QT)
            sums[b, :, cols] = own_sum[b, :, d * QT : (d + 1) * QT]

    def mirror(group, d, other):
        to_core = lax.rem(core + other, 2)
        return pltpu.make_async_remote_copy(
            mirror_out.at[group, d - 1, to_core],
            mirror_in.at[group, d - 1, pl.ds(pl.multiple_of(core * 64, 64), 64), :],
            mir_send.at[group, d - 1, other], mir_recv.at[group, d - 1, other],
            device_id={"dp": strip_of(d), "outer": to_core}, device_id_type=MESH,
        )

    def send_mirror(group):
        low = lax.broadcasted_iota(jnp.int32, (64, QT), 1) < 64
        for d in (1, 2, 3):
            cols = slice(d * QT, (d + 1) * QT)
            if group == 0:
                one, two = own_sum[0, :, cols], own_sum[1, :, cols]
                pair = (
                    jnp.where(low, one, pltpu.roll(two, 64, 1)),
                    jnp.where(low, pltpu.roll(one, 64, 1), two),
                )
            else:
                pair = (own_sum[2, :, cols],) * 2
            for half in range(2):
                mirror_out[group, d - 1, half] = pair[half].astype(jnp.bfloat16)
        for d in (1, 2, 3):
            for other in range(2):
                mirror(group, d, other).start()

    def take_mirror(group):
        for d in (1, 2, 3):
            for other in range(2):
                mirror(group, d, other).wait()
        for d in (1, 2, 3):
            cols = pl.ds(pl.multiple_of(strip_of(STRIPS - d) * QT, QT), QT)
            flipped = wide(mirror_in[group, d - 1]).T
            if group == 0:
                sums[0, :, cols] = flipped[:64]
                sums[1, :, cols] = flipped[64:]
            else:
                turned[...] = flipped
                sums[2, :, cols] = turned[pl.ds(pl.multiple_of(core * 64, 64), 64), :]

    def first(k, carry):
        load(0, k).wait()
        dequantize(0, k)
        return carry

    lax.fori_loop(0, chunks, first, 0)
    for k in range(chunks):
        load(2, k).start()

    for b in range(NB):

        def step(j, carry):
            if b > 0:

                @pl.when(j == 1)
                def _():
                    chip_sum(b - 1)
                    if b == 1:
                        g_far.wait()
                        for o in AROUND:
                            g_next[o - 1].start()

            if b == 0:

                @pl.when(j == 2)
                def _():
                    a_far.wait()
                    for o in (0, 2, 1):
                        a_next[o].start()

            if b + 1 < NB:
                load(b + 1, j).wait()
            gram(b, j)
            if b + 1 < NB:
                dequantize(b + 1, j)
            return carry

        lax.fori_loop(0, 4, step, 0)
        swap(b).start()
    second(0)
    chip_sum(NB - 1)
    second(NB - 2)
    finish(0)

    a_pair.append(a_copy(z_far(dp), core, 8, {"outer": 1 - core}))
    a_pair[-1].start()
    for o in (1, 2, 3):
        a_near[o - 1].wait()
        a_pair.append(a_copy(y_peer(4 - o), core, 8 + o, {"outer": 1 - core}))
        a_pair[-1].start()
    for o in (1, 2, 3):
        a_next[o - 1].wait()
        a_pair.append(a_copy(z_far(y_peer(4 - o)), core, 11 + o, {"outer": 1 - core}))
        a_pair[-1].start()

    def precondition(n):
        cols = pl.ds(n * 512, 512)
        right[...] = jnp.dot(
            weight[...], g_full[:, cols], preferred_element_type=jnp.float32
        ).astype(jnp.bfloat16)
        pre_out[:, cols] = jnp.dot(
            a_full[...], right[...], preferred_element_type=jnp.float32
        ).astype(jnp.bfloat16)

    second(NB - 1)
    finish(1)
    send_mirror(0)
    own_w.wait()
    for o in (1, 2, 3):
        g_near[o - 1].wait()
        g_next[o - 1].wait()
    for copy in a_pair:
        copy.wait()
    precondition(0)
    finish(2)
    send_mirror(1)
    precondition(1)
    take_mirror(0)
    take_mirror(1)
    a_out[0] = sums[0]
    g_out[0] = sums[1]
    g_out[1] = sums[2]


def blend(token_total, a_sum, g_sum, pre, prior, factor, a_stat, g_stat, new_a, new_g, pre_out, sem):
    copy = pltpu.make_async_copy(pre, pre_out, sem)
    copy.start()
    for total, old, stat, new in ((a_sum, prior, a_stat, new_a), (g_sum, factor, g_stat, new_g)):
        mean = total[...] / token_total
        stat[...] = mean
        new[...] = EMA_DECAY * old[...] + (1.0 - EMA_DECAY) * mean
    copy.wait()


def body(
    activations,
    act_scale,
    out_grads,
    gradient_tile_scale,
    prior_input_factor,
    g_factor,
    weight_grad,
    a_inverse,
    g_inverse,
):
    tokens = activations.shape[0]
    token_total = tokens * lax.axis_size("dp") * lax.axis_size("outer")
    vmem = pl.BlockSpec(memory_space=pltpu.VMEM)
    hbm = pl.BlockSpec(memory_space=pltpu.HBM)
    bf16, f32 = jnp.bfloat16, jnp.float32
    dma = pltpu.SemaphoreType.DMA
    a_sum, g_sum, preconditioned = pl.pallas_call(
        kernel,
        out_shape=(
            jax.ShapeDtypeStruct((1, 64, BLK), f32),
            jax.ShapeDtypeStruct((2, 64, BLK), f32),
            jax.ShapeDtypeStruct((BLK, BLK), bf16),
        ),
        in_specs=[hbm] * 7,
        out_specs=(vmem, vmem, vmem),
        scratch_shapes=[
            pltpu.SMEM(act_scale.shape[::-1], f32),
            pltpu.SMEM(gradient_tile_scale.shape, f32),
            pltpu.VMEM((2, tokens, BLK), bf16),
            pltpu.VMEM((tokens, BLK), bf16),
            pltpu.VMEM((tokens, BLK), bf16),
            pltpu.VMEM((12 * QT, tokens), bf16),
            pltpu.VMEM((12 * QT, tokens), bf16),
            pltpu.VMEM((2, NB, STRIPS, 64, WIDE), bf16),
            pltpu.VMEM((NB, STRIPS, 64, WIDE), bf16),
            pltpu.VMEM((NB, 2, 4, 64, WIDE), bf16),
            pltpu.VMEM((NB, 3, 2, 64, 2 * QT), bf16),
            pltpu.VMEM((NB, 4, 64, WIDE - 2 * QT), bf16),
            pltpu.VMEM((NB, 2, 64, 2 * QT), bf16),
            pltpu.VMEM((NB, 4, 64, WIDE - 2 * QT), bf16),
            pltpu.VMEM((NB, 64, 2 * QT), bf16),
            pltpu.VMEM((NB, 3, 64, WIDE - 2 * QT), bf16),
            pltpu.VMEM((NB, 64, WIDE), f32),
            pltpu.VMEM((NB, 64, BLK), f32),
            pltpu.VMEM((2, 3, 2, 64, QT), bf16),
            pltpu.VMEM((2, 3, QT, QT), bf16),
            pltpu.VMEM((QT, QT), f32),
            pltpu.VMEM((BLK, BLK), bf16),
            pltpu.VMEM((BLK, BLK), bf16),
            pltpu.VMEM((BLK, BLK), bf16),
            pltpu.VMEM((BLK, 512), bf16),
            dma((NB, tokens // CHUNK)),
            dma((5,)),
            dma((7,)),
            dma((7,)),
            dma((15,)),
            dma((15,)),
            dma((NB,)),
            dma((NB,)),
            dma((NB, 4)),
            dma((NB, 4)),
            dma((NB, 4)),
            dma((NB, 4)),
            dma((2, 3, 2)),
            dma((2, 3, 2)),
        ],
        compiler_params=pltpu.CompilerParams(
            collective_id=0, has_side_effects=True, vmem_limit_bytes=50 << 20
        ),
        cost_estimate=pl.CostEstimate(
            flops=14_000_000_000, bytes_accessed=20_000_000, transcendentals=0
        ),
    )(
        *(
            pltpu.with_memory_space_constraint(value, pltpu.HBM)
            for value in (
                act_scale.T,
                gradient_tile_scale,
                activations,
                out_grads,
                weight_grad,
                a_inverse,
                g_inverse,
            )
        )
    )
    return pl.pallas_call(
        functools.partial(blend, token_total),
        out_shape=(
            jax.ShapeDtypeStruct((1, 64, BLK), f32),
            jax.ShapeDtypeStruct((2, 64, BLK), f32),
            jax.ShapeDtypeStruct((1, 64, BLK), f32),
            jax.ShapeDtypeStruct((2, 64, BLK), f32),
            jax.ShapeDtypeStruct((BLK, BLK), bf16),
        ),
        in_specs=[vmem] * 5,
        out_specs=(vmem, vmem, vmem, vmem, hbm),
        scratch_shapes=[dma],
        compiler_params=pltpu.CompilerParams(vmem_limit_bytes=8 << 20),
    )(a_sum, g_sum, preconditioned, prior_input_factor, g_factor)


def solution(mesh):
    return jax.shard_map(
        body,
        mesh=mesh,
        in_specs=(
            P(("dp", "outer"), "mp"),
            P(("dp", "outer"), "mp"),
            P(("dp", "outer"), "mp"),
            P(("dp", "outer"), "mp"),
            P("mp", ("dp", "outer"), None),
            P("mp", ("dp", "outer"), None),
            P("mp", ("dp", "outer")),
            P("mp", ("dp", "outer"), None),
            P(("dp", "outer"), "mp", None),
        ),
        out_specs=(
            P("mp", ("dp", "outer"), None),
            P("mp", ("dp", "outer"), None),
            P("mp", ("dp", "outer"), None),
            P("mp", ("dp", "outer"), None),
            P("mp", ("dp", "outer")),
        ),
        check_vma=False,
    )
```
